32 devices in a mesh: expert: 4 (over y, core), shard: 8 (over z, x).
Axes of the slice: x: 2, y: 2, z: 4, core: 2. Of those that a mesh axis runs over, the one named last changes fastest.
Arguments:
- train_down: float32 [16, 6400, 4096], P('expert', None, 'shard'), may hold values from -0.109375 to 0.109375
- other_down: bfloat16 [16, 6400, 4096], P('expert', None, 'shard'), may hold values from -0.0390625 to 0.0390625
- router_weight: float32 [4096, 16], P('shard', 'expert'), may hold values from -0.09375 to 0.09375
- router_gain: float32 [4096], P('shard'), may hold values from 0.25 to 1.75
Outputs:
- ready_down: bfloat16 [16, 6400, 4096], P('expert', 'shard')
- scale_down: float32 [16, 6400], P('expert', 'shard')
- serve_router: bfloat16 [4096, 16], replicated
The draws below stay inside these ranges and needn't reach their ends.
All inputs are finite; a program needn't handle non-finite values.
Results may differ from the reference program's by a relative error of at most 0.001.
Values may be sent and summed in bfloat16 or wider, within the bound.
A program may use at most 256 MiB of HBM per device.

```python
import jax
import jax.numpy as jnp
from jax import lax

EXPERTS = 16
D_MODEL = 4096
D_EXPERT = 6400


def with_spikes(array, rng, source, target, parts, factor):
    def block_of(axis_at):
        return (jnp.arange(array.shape[axis_at]) // (array.shape[axis_at] // parts)).reshape((-1,) + (1,) * (array.ndim - 1 - axis_at))

    first = jax.random.permutation(rng, parts)[block_of(target)]
    far = (block_of(target) + parts // 2) % parts
    return jnp.where((block_of(source) == first) | (block_of(source) == far), factor * array, array)


def block_levels(own_key, shape, cuts, low, high):
    gain = 1.0
    for axis_at, shards_of in cuts:
        steps = jax.random.uniform(jax.random.fold_in(jax.random.fold_in(own_key, 6), axis_at), (shards_of,), jnp.float32, low / len(cuts), high / len(cuts))
        gain = gain * jnp.repeat(jnp.exp(steps), shape[axis_at] // shards_of).reshape((-1,) + (1,) * (len(shape) - 1 - axis_at))
    return gain


def centred(rng, extent, deviation, bound, shards=(), held_as=jnp.bfloat16):
    result = jax.random.normal(rng, extent, jnp.float32) * deviation
    if len(shards) > 0:
        result = block_levels(rng, extent, shards, -0.22, 0.18) * result
    return jnp.clip(result, min=-bound, max=bound).astype(held_as)


def bell_draw_with(key, dims, deviation, reach, pieces, heavy, held_as=jnp.bfloat16):
    entries = deviation * jax.random.normal(key, dims, jnp.float32)
    if pieces:
        entries = entries * block_levels(key, dims, pieces, -0.22, 0.18)
    return jnp.clip(with_spikes(entries, jax.random.fold_in(key, 3), *heavy), -reach, reach).astype(held_as)


def setup_inputs(seed: int = 0) -> dict:
    key_of = jax.random.split(jax.random.key(seed), 5)
    return {
        "train_down": bell_draw_with(key_of[0], (EXPERTS, D_EXPERT, D_MODEL), D_EXPERT ** -0.5, 0.109375, ((0, 4), (2, 8)), (2, 1, 8, 2.0), jnp.float32),
        "other_down": centred(key_of[1], (EXPERTS, D_EXPERT, D_MODEL), (D_EXPERT * 4) ** -0.5, 0.0390625, ((0, 4), (2, 8))),
        "router_weight": centred(key_of[2], (D_MODEL, EXPERTS), D_MODEL ** -0.5, 0.09375, ((0, 8), (1, 4)), jnp.float32),
        "router_gain": jnp.clip(1.0 + 0.15 * jax.random.normal(key_of[3], (D_MODEL,), jnp.float32), 0.25, 1.75),
    }


def reference(train_down, other_down, router_weight, router_gain):
    latest_down = train_down + other_down.astype(jnp.float32)
    scale_down = jnp.sqrt(lax.optimization_barrier(jnp.sum(latest_down * latest_down, axis=2)))
    ready_down = (latest_down / jnp.expand_dims(scale_down, 2)).astype(jnp.bfloat16)
    serve_router = (router_weight * router_gain[:, None]).astype(jnp.bfloat16)
    return (ready_down, scale_down, serve_router)
```

```python
import functools

import jax
import jax.numpy as jnp
from jax import lax
from jax.experimental import pallas as pl
from jax.experimental.pallas import tpu as pltpu
from jax.sharding import PartitionSpec as P

LANES = 128
RING = 4
SLOTS = 6


def unit_rows(rows):
    fits = [r for r in range(16, LANES + 1, 16) if rows % r == 0]
    return fits[-1] if fits else rows


def rows_to_lanes(column_sums):
    rows = column_sums.shape[0]
    out = []
    for start in range(0, rows, LANES):
        block = column_sums[start : min(start + LANES, rows)]
        if block.shape[0] < LANES:
            fill = jnp.zeros((LANES - block.shape[0], LANES), block.dtype)
            block = jnp.concatenate([block, fill], axis=0)
        out.append(jnp.sum(block.T, axis=0, keepdims=True))
    return jnp.concatenate(out, axis=1) if len(out) > 1 else out[0]


def lanes_to_rows(row, rows):
    out = []
    for start in range(0, rows, LANES):
        block = jnp.broadcast_to(row[:, start : start + LANES], (LANES, LANES)).T
        out.append(block[: min(LANES, rows - start)])
    return jnp.concatenate(out, axis=0) if len(out) > 1 else out[0]


def update_kernel(
    n, ne, r,
    train_ref, other_ref, weight_ref, gain_ref,
    ready_ref, scale_ref, router_ref,
    train_buf, other_buf, stage, part, first, half_sum, far_sum, recip,
    train_sem, other_sem, stage_sem, data_sem,
    small_sem, first_sem, far_sem, recip_sem,
    router_send, router_row_sem, router_col_sem,
):
    experts, _, rows, width = train_ref.shape
    steps = rows // r
    units = experts * steps
    half = n // 2
    me, my_e = lax.axis_index("shard"), lax.axis_index("expert")
    place, side = lax.rem(me, half), lax.div(me, half)

    def shard(d):
        return {"device_id": {"shard": d}, "device_id_type": pl.DeviceIdType.MESH}

    def expert(d):
        return {"device_id": {"expert": d}, "device_id_type": pl.DeviceIdType.MESH}

    def where_is(k):
        start = lax.rem(k, steps) * r
        return lax.div(k, steps), pl.ds(pl.multiple_of(start, 8), r)

    def columns_of(d):
        return pl.ds(pl.multiple_of(d * width, LANES), width)

    def loads(k):
        e, at = where_is(k)
        slot = lax.rem(k, SLOTS)
        return (
            pltpu.make_async_copy(
                train_ref.at[e, :, at, :], train_buf.at[slot], train_sem.at[slot]
            ),
            pltpu.make_async_copy(
                other_ref.at[e, :, at, :], other_buf.at[slot], other_sem.at[slot]
            ),
        )

    def start_loads(k):
        for copy in loads(k):
            copy.start()

    start_loads(0)
    if units > 1:
        start_loads(1)

    mine = columns_of(me)
    router_ref[my_e, :, mine] = (weight_ref[...] * gain_ref[...]).astype(router_ref.dtype)

    barrier = pltpu.get_barrier_semaphore()
    for j in range(1, n):
        pl.semaphore_signal(barrier, inc=1, **shard(lax.rem(me + j, n)))
    for j in range(1, ne):
        pl.semaphore_signal(barrier, inc=1, **expert(lax.rem(my_e + j, ne)))
    pl.semaphore_wait(barrier, n + ne - 2)

    def latest(slot, d):
        return train_buf[slot, d] + other_buf[slot, d].astype(jnp.float32)

    def sum_own(k):
        for copy in loads(k):
            copy.wait()
        slot = lax.rem(k, SLOTS)

        def body(q, carry):
            pair = []
            for t in (0, 1):
                x = latest(slot, t * half + q)
                x = x * x
                total = x[:, :LANES]
                for at in range(LANES, width, LANES):
                    total = total + x[:, at : at + LANES]
                pair.append(rows_to_lanes(total))
            part[k, q] = jnp.concatenate(pair, axis=0)
            return carry

        lax.fori_loop(0, half, body, 0)
        first[k, place] = part[k, place]
        for j in range(1, half):
            q = lax.rem(place + j, half)
            pltpu.make_async_remote_copy(
                src_ref=part.at[k, q],
                dst_ref=first.at[k, place],
                send_sem=small_sem.at[0],
                recv_sem=first_sem.at[k],
                **shard(side * half + q),
            ).start()

    def few(ref, k):
        return ref.at[k, pl.ds(0, half - 1)]

    def sum_half(k):
        pltpu.make_async_remote_copy(
            few(first, k), few(first, k), small_sem.at[0], first_sem.at[k], **shard(me)
        ).wait_recv()
        total = first[k, 0]
        for q in range(1, half):
            total = total + first[k, q]
        half_sum[k] = total
        pltpu.make_async_remote_copy(
            src_ref=half_sum.at[k],
            dst_ref=far_sum.at[k],
            send_sem=small_sem.at[1],
            recv_sem=far_sem.at[k],
            **shard((1 - side) * half + place),
        ).start()

    def sum_all(k):
        pltpu.make_async_remote_copy(
            far_sum.at[k], far_sum.at[k], small_sem.at[1], far_sem.at[k], **shard(me)
        ).wait_recv()
        scale = jnp.sqrt(half_sum[k] + far_sum[k])
        scale_ref[k] = jnp.where(side == 0, scale[0:1], scale[1:2])
        recip[k, place] = 1.0 / scale
        for j in range(1, half):
            q = lax.rem(place + j, half)
            pltpu.make_async_remote_copy(
                src_ref=recip.at[k, place],
                dst_ref=recip.at[k, place],
                send_sem=small_sem.at[2],
                recv_sem=recip_sem.at[k],
                **shard(side * half + q),
            ).start()

    def wait_stage(slot):
        some = stage.at[slot, pl.ds(0, n - 1)]
        pltpu.make_async_remote_copy(
            some, some, stage_sem.at[slot], data_sem.at[0], **shard(me)
        ).wait_send()

    def send(k):
        pltpu.make_async_remote_copy(
            few(recip, k), few(recip, k), small_sem.at[2], recip_sem.at[k], **shard(me)
        ).wait_recv()
        slot, ring = lax.rem(k, SLOTS), lax.rem(k, RING)
        e, at = where_is(k)

        @pl.when(k >= RING)
        def _():
            wait_stage(ring)

        def target(m):
            far = m < half
            t = jnp.where(far, 1 - side, side)
            q = lax.rem(place + jnp.where(far, m, m - half + 1), half)
            return t, q

        def piece(t, q):
            pair = recip[k, q]
            row = jnp.where(t == 0, pair[0:1], pair[1:2])
            factor = lanes_to_rows(row, r)
            factor = jnp.concatenate([factor] * (width // LANES), axis=1)
            return (latest(slot, t * half + q) * factor).astype(stage.dtype)

        def copy_to(m):
            t, q = target(m)
            return pltpu.make_async_remote_copy(
                src_ref=stage.at[ring, m],
                dst_ref=ready_ref.at[e, at, mine],
                send_sem=stage_sem.at[ring],
                recv_sem=data_sem.at[me],
                **shard(t * half + q),
            )

        def body(m, carry):
            stage[ring, m] = piece(*target(m))

            @pl.when(m > 0)
            def _():
                copy_to(m - 1).start()

            return carry

        lax.fori_loop(0, n - 1, body, 0)
        ready_ref[e, at, mine] = piece(side, place)
        copy_to(n - 2).start()

    for j in range(1, n):
        pltpu.make_async_remote_copy(
            src_ref=router_ref.at[my_e, :, mine],
            dst_ref=router_ref.at[my_e, :, mine],
            send_sem=router_send.at[0],
            recv_sem=router_row_sem,
            **shard(lax.rem(me + j, n)),
        ).start()

    def step(i, carry):
        @pl.when(i + 2 < units)
        def _():
            start_loads(i + 2)

        @pl.when(i < units)
        def _():
            sum_own(i)

        @pl.when((i >= 1) & (i < units + 1))
        def _():
            sum_half(i - 1)

        @pl.when((i >= 2) & (i < units + 2))
        def _():
            sum_all(i - 2)

        @pl.when(i >= 3)
        def _():
            send(i - 3)

        return carry

    lax.fori_loop(0, units + 3, step, 0)

    others = router_ref.at[0, :, pl.ds(0, (n - 1) * width)]
    pltpu.make_async_remote_copy(
        others, others, router_send.at[0], router_row_sem, **shard(me)
    ).wait()
    for j in range(1, ne):
        pltpu.make_async_remote_copy(
            src_ref=router_ref.at[my_e],
            dst_ref=router_ref.at[my_e],
            send_sem=router_send.at[1],
            recv_sem=router_col_sem,
            **expert(lax.rem(my_e + j, ne)),
        ).start()

    for slot in range(min(RING, units)):
        wait_stage(slot)
    for j in range(1, n):
        d = lax.rem(me + j, n)
        there = ready_ref.at[:, :, columns_of(d)]
        pltpu.make_async_remote_copy(
            there, there, stage_sem.at[0], data_sem.at[d], **shard(me)
        ).wait_recv()
    sent = part.at[:, pl.ds(0, half - 1)]
    for at in (0, 2):
        pltpu.make_async_remote_copy(
            sent, sent, small_sem.at[at], data_sem.at[0], **shard(me)
        ).wait_send()
    pltpu.make_async_remote_copy(
        half_sum, half_sum, small_sem.at[1], data_sem.at[0], **shard(me)
    ).wait_send()
    others = router_ref.at[pl.ds(0, ne - 1)]
    pltpu.make_async_remote_copy(
        others, others, router_send.at[1], router_col_sem, **shard(me)
    ).wait()


def update(train_down, other_down, weight, gain, n, ne):
    experts, inner, width = train_down.shape
    rows = inner // n
    r = unit_rows(rows)
    units = experts * (rows // r)
    lanes = -(-r // LANES) * LANES
    half = n // 2
    f32, bf16 = jnp.float32, jnp.bfloat16
    dma = pltpu.SemaphoreType.DMA
    return pl.pallas_call(
        functools.partial(update_kernel, n, ne, r),
        out_shape=(
            pltpu.VMEM((experts, rows, width * n), bf16),
            pltpu.VMEM((units, 1, lanes), f32),
            pltpu.VMEM((ne, weight.shape[0], width * n), bf16),
        ),
        in_specs=[
            pl.BlockSpec(memory_space=pl.ANY),
            pl.BlockSpec(memory_space=pl.ANY),
            pl.BlockSpec(memory_space=pltpu.VMEM),
            pl.BlockSpec(memory_space=pltpu.VMEM),
        ],
        out_specs=(pl.BlockSpec(memory_space=pltpu.VMEM),) * 3,
        scratch_shapes=[
            pltpu.VMEM((SLOTS, n, r, width), f32),
            pltpu.VMEM((SLOTS, n, r, width), bf16),
            pltpu.VMEM((RING, n - 1, r, width), bf16),
            pltpu.VMEM((units, half, 2, lanes), f32),
            pltpu.VMEM((units, half, 2, lanes), f32),
            pltpu.VMEM((units, 2, lanes), f32),
            pltpu.VMEM((units, 2, lanes), f32),
            pltpu.VMEM((units, half, 2, lanes), f32),
            dma((SLOTS,)),
            dma((SLOTS,)),
            dma((RING,)),
            dma((n,)),
            dma((3,)),
            dma((units,)),
            dma((units,)),
            dma((units,)),
            dma((2,)),
            dma,
            dma,
        ],
        compiler_params=pltpu.CompilerParams(
            collective_id=0, has_side_effects=True, vmem_limit_bytes=36 * 2**20
        ),
        name="update",
    )(
        train_down.reshape(experts, n, rows, width),
        other_down.reshape(experts, n, rows, width),
        weight,
        gain,
    )


def settle_kernel(
    ready_ref, scale_ref, router_ref, ready_out, scale_out, router_out, ready_sem
):
    copies = [
        pltpu.make_async_copy(ready_ref.at[e], ready_out.at[e], ready_sem.at[e])
        for e in range(ready_ref.shape[0])
    ]
    for copy in copies:
        copy.start()
    scale_out[...] = scale_ref[...]
    router_out[...] = router_ref[...]
    for copy in copies:
        copy.wait()


def settle(ready_down, scale, router):
    vmem = pl.BlockSpec(memory_space=pltpu.VMEM)
    return pl.pallas_call(
        settle_kernel,
        out_shape=tuple(
            jax.ShapeDtypeStruct(x.shape, x.dtype) for x in (ready_down, scale, router)
        ),
        in_specs=[vmem] * 3,
        out_specs=(pl.BlockSpec(memory_space=pl.ANY), vmem, vmem),
        scratch_shapes=[pltpu.SemaphoreType.DMA((ready_down.shape[0],))],
        compiler_params=pltpu.CompilerParams(vmem_limit_bytes=8 * 2**20),
        name="settle",
    )(pltpu.with_memory_space_constraint(ready_down, pltpu.VMEM), scale, router)


def per_device(n, ne, train_down, other_down, router_weight, router_gain):
    experts, inner, width = train_down.shape
    rows = inner // n
    r = unit_rows(rows)
    ready_down, scale, router = update(
        train_down, other_down, router_weight.T, router_gain[None, :], n, ne
    )
    ready_down, scale, router = settle(ready_down, scale, router)
    scale_down = scale.reshape(experts, rows // r, -1)[:, :, :r].reshape(experts, rows)
    serve_router = router.reshape(-1, width * n).T
    return (ready_down, scale_down, serve_router)


def solution(mesh):
    in_specs = (
        P("expert", None, "shard"),
        P("expert", None, "shard"),
        P("shard", "expert"),
        P("shard"),
    )
    out_specs = (P("expert", "shard", None), P("expert", "shard"), P())
    return jax.shard_map(
        functools.partial(per_device, mesh.shape["shard"], mesh.shape["expert"]),
        mesh=mesh,
        in_specs=in_specs,
        out_specs=out_specs,
        check_vma=False,
    )
```

```python
import functools

import jax
import jax.numpy as jnp
from jax import lax
from jax.experimental import pallas as pl
from jax.experimental.pallas import tpu as pltpu
from jax.sharding import PartitionSpec as P

LANES = 128
UNIT = 128
RING = 4
GROUP = 4
LAGS = (7, 4, 2)


def unit_rows(rows):
    fits = [r for r in range(16, UNIT + 1, 16) if rows % r == 0]
    return fits[-1] if fits else rows


def rows_to_lanes(column_sums):
    rows = column_sums.shape[0]
    out = []
    for start in range(0, rows, LANES):
        block = column_sums[start : min(start + LANES, rows)]
        if block.shape[0] < LANES:
            fill = jnp.zeros((LANES - block.shape[0], LANES), block.dtype)
            block = jnp.concatenate([block, fill], axis=0)
        out.append(jnp.sum(block.T, axis=0, keepdims=True))
    return jnp.concatenate(out, axis=1) if len(out) > 1 else out[0]


def lanes_to_rows(row, rows):
    out = []
    for start in range(0, rows, LANES):
        block = jnp.broadcast_to(row[:, start : start + LANES], (LANES, LANES)).T
        out.append(block[: min(LANES, rows - start)])
    return jnp.concatenate(out, axis=0) if len(out) > 1 else out[0]


def update_kernel(
    n, ne, r, head,
    train_ref, other_ref, weight_ref, gain_ref,
    ready_ref, scale_ref, router_ref,
    train_buf, other_buf, stage, part, direct, first, half_sum, far_sum, recip,
    train_sem, other_sem, stage_sem, data_sem,
    small_sem, direct_sem, first_sem, far_sem, recip_sem,
    router_send, router_row_sem, router_col_sem,
):
    experts, _, rows, width = train_ref.shape
    steps = rows // r
    units = experts * steps
    groups = (units - head) // GROUP
    half = n // 2
    me, my_e = lax.axis_index("shard"), lax.axis_index("expert")
    place, side = lax.rem(me, half), lax.div(me, half)

    def shard(d):
        return {"device_id": {"shard": d}, "device_id_type": pl.DeviceIdType.MESH}

    def expert(d):
        return {"device_id": {"expert": d}, "device_id_type": pl.DeviceIdType.MESH}

    def wait_recv(ref, sem):
        pltpu.make_async_remote_copy(ref, ref, small_sem.at[0], sem, **shard(me)).wait_recv()

    def wait_send(ref, sem):
        pltpu.make_async_remote_copy(ref, ref, sem, data_sem.at[0], **shard(me)).wait_send()

    def where_is(k):
        start = lax.rem(k, steps) * r
        return lax.div(k, steps), pl.ds(pl.multiple_of(start, 8), r)

    def columns_of(d):
        return pl.ds(pl.multiple_of(d * width, LANES), width)

    def loads(k, slot):
        e, at = where_is(k)
        return (
            pltpu.make_async_copy(
                train_ref.at[e, :, at, :], train_buf.at[slot], train_sem.at[slot]
            ),
            pltpu.make_async_copy(
                other_ref.at[e, :, at, :], other_buf.at[slot], other_sem.at[slot]
            ),
        )

    def start_loads(k, slot):
        for copy in loads(k, slot):
            copy.start()

    def wait_loads(k, slot):
        for copy in loads(k, slot):
            copy.wait()

    def sum_slot(k):
        return lax.rem(k, GROUP)

    def send_slot(k):
        return GROUP + lax.rem(k, 3)

    start_loads(0, 0)
    if units > 1:
        start_loads(1, 1)

    mine = columns_of(me)
    router_ref[my_e, :, mine] = (weight_ref[...] * gain_ref[...]).astype(router_ref.dtype)

    barrier = pltpu.get_barrier_semaphore()
    for j in range(1, n):
        pl.semaphore_signal(barrier, inc=1, **shard(lax.rem(me + j, n)))
    for j in range(1, ne):
        pl.semaphore_signal(barrier, inc=1, **expert(lax.rem(my_e + j, ne)))
    pl.semaphore_wait(barrier, n + ne - 2)

    def latest(slot, d):
        return train_buf[slot, d] + other_buf[slot, d].astype(jnp.float32)

    def sum_own(k):
        slot = sum_slot(k)
        wait_loads(k, slot)

        def body(q, carry):
            pair = []
            for t in (0, 1):
                x = latest(slot, t * half + q)
                x = x * x
                total = x[:, :LANES]
                for at in range(LANES, width, LANES):
                    total = total + x[:, at : at + LANES]
                pair.append(rows_to_lanes(total))
            part[q, k] = jnp.concatenate(pair, axis=0)
            return carry

        lax.fori_loop(0, half, body, 0)

    def own_side(pair):
        return jnp.where(side == 0, pair[..., 0:1, :], pair[..., 1:2, :])

    def send_direct(k):
        for q in range(half):
            direct[k, me, q] = part[q, k]
        for j in range(1, n):
            pltpu.make_async_remote_copy(
                src_ref=part.at[:, k],
                dst_ref=direct.at[k, me],
                send_sem=small_sem.at[3],
                recv_sem=direct_sem.at[k],
                **shard(lax.rem(me + (half + j - 1 if j <= half else j - half), n)),
            ).start()

    def sum_direct(k):
        wait_recv(direct.at[k, pl.ds(0, n - 1)], direct_sem.at[k])
        for q in range(half):
            total = direct[k, 0, q]
            for s in range(1, n):
                total = total + direct[k, s, q]
            scale = jnp.sqrt(total)
            recip[q, k] = 1.0 / scale

            @pl.when(place == q)
            def _(scale=scale):
                scale_ref[k] = own_side(scale)

    def units_of(g):
        return pl.ds(head + g * GROUP, GROUP)

    def sum_group(g):
        at = units_of(g)

        def body(j, carry):
            k = head + g * GROUP + j
            sum_own(k)

            @pl.when(k + GROUP < units)
            def _():
                start_loads(k + GROUP, sum_slot(k))

            return carry

        lax.fori_loop(0, GROUP, body, 0)
        first[place, at] = part[place, at]
        for j in range(1, half):
            q = lax.rem(place + j, half)
            pltpu.make_async_remote_copy(
                src_ref=part.at[q, at],
                dst_ref=first.at[place, at],
                send_sem=small_sem.at[0],
                recv_sem=first_sem.at[g],
                **shard(side * half + q),
            ).start()

    def sum_half(g):
        at = units_of(g)
        wait_recv(first.at[pl.ds(0, half - 1), at], first_sem.at[g])
        total = first[0, at]
        for q in range(1, half):
            total = total + first[q, at]
        half_sum[at] = total
        pltpu.make_async_remote_copy(
            src_ref=half_sum.at[at],
            dst_ref=far_sum.at[at],
            send_sem=small_sem.at[1],
            recv_sem=far_sem.at[g],
            **shard((1 - side) * half + place),
        ).start()

    def sum_all(g):
        at = units_of(g)
        wait_recv(far_sum.at[at], far_sem.at[g])
        scale = jnp.sqrt(half_sum[at] + far_sum[at])
        scale_ref[at] = own_side(scale)
        recip[place, at] = 1.0 / scale
        for j in range(1, half):
            q = lax.rem(place + j, half)
            pltpu.make_async_remote_copy(
                src_ref=recip.at[place, at],
                dst_ref=recip.at[place, at],
                send_sem=small_sem.at[2],
                recv_sem=recip_sem.at[g],
                **shard(side * half + q),
            ).start()

    def wait_stage(slot):
        wait_send(stage.at[slot, pl.ds(0, n - 1)], stage_sem.at[slot])

    def send(k):
        slot, ring = send_slot(k), lax.rem(k, RING)
        e, at = where_is(k)
        wait_loads(k, slot)

        @pl.when(k >= RING)
        def _():
            wait_stage(ring)

        def target(m):
            m = lax.rem(m + jnp.where(k == 0, 0, half), n - 1)
            far = m < half
            t = jnp.where(far, 1 - side, side)
            q = lax.rem(place + jnp.where(far, m, m - half + 1), half)
            return t, q

        def piece(t, q):
            pair = recip[q, k]
            row = jnp.where(t == 0, pair[0:1], pair[1:2])
            factor = lanes_to_rows(row, r)
            factor = jnp.concatenate([factor] * (width // LANES), axis=1)
            return (latest(slot, t * half + q) * factor).astype(stage.dtype)

        def copy_to(m):
            t, q = target(m)
            return pltpu.make_async_remote_copy(
                src_ref=stage.at[ring, m],
                dst_ref=ready_ref.at[e, at, mine],
                send_sem=stage_sem.at[ring],
                recv_sem=data_sem.at[me],
                **shard(t * half + q),
            )

        def body(m, carry):
            stage[ring, m] = piece(*target(m))

            @pl.when(m > 0)
            def _():
                copy_to(m - 1).start()

            return carry

        lax.fori_loop(0, n - 1, body, 0)
        ready_ref[e, at, mine] = piece(side, place)
        copy_to(n - 2).start()

    for k in range(head):
        sum_own(k)
        send_direct(k)
        if k < min(3, units):
            start_loads(k, send_slot(k))
        if k + 2 < min(GROUP, units):
            start_loads(k + 2, k + 2)
        if k + GROUP < head:
            start_loads(k + GROUP, k)
    for k in range(head, min(head + GROUP, units)):
        start_loads(k, sum_slot(k))

    def step(i, carry):
        def at_lag(lag, start):
            g = jnp.where(i == start, 0, lax.div(i + lag - head, GROUP))
            due = (i == start) | (
                (i + lag >= head + GROUP) & (lax.rem(i + lag - head, GROUP) == 0)
            )
            return g, due & (g < groups)

        if groups > 0:
            g, due = at_lag(LAGS[2], 3)

            @pl.when(due)
            def _():
                sum_all(g)

            g, due = at_lag(LAGS[1], 2)

            @pl.when(due)
            def _():
                sum_half(g)

        @pl.when(i < head)
        def _():
            sum_direct(i)

        if groups > 0:

            @pl.when((i >= head) & (lax.rem(i - head, GROUP) == 0))
            def _():
                g = lax.div(i - head, GROUP)
                wait_recv(recip.at[pl.ds(0, half - 1), units_of(g)], recip_sem.at[g])

        send(i)

        @pl.when(i + 3 < units)
        def _():
            start_loads(i + 3, send_slot(i))

        if groups > 0:
            g, due = at_lag(LAGS[0], 0)

            @pl.when(due)
            def _():
                sum_group(g)

        return carry

    def send_router():
        for j in range(1, n):
            pltpu.make_async_remote_copy(
                src_ref=router_ref.at[my_e, :, mine],
                dst_ref=router_ref.at[my_e, :, mine],
                send_sem=router_send.at[0],
                recv_sem=router_row_sem,
                **shard(lax.rem(me + j, n)),
            ).start()

    lax.fori_loop(0, 1, step, 0)
    send_router()
    lax.fori_loop(1, units, step, 0)

    others = router_ref.at[0, :, pl.ds(0, (n - 1) * width)]
    pltpu.make_async_remote_copy(
        others, others, router_send.at[0], router_row_sem, **shard(me)
    ).wait()
    for j in range(1, ne):
        pltpu.make_async_remote_copy(
            src_ref=router_ref.at[my_e],
            dst_ref=router_ref.at[my_e],
            send_sem=router_send.at[1],
            recv_sem=router_col_sem,
            **expert(lax.rem(my_e + j, ne)),
        ).start()

    for slot in range(min(RING, units)):
        wait_stage(slot)
    wait_send(direct.at[:, pl.ds(0, n - 1)], small_sem.at[3])
    if groups > 0:
        late = pl.ds(head, groups * GROUP)
        wait_send(part.at[pl.ds(0, half - 1), late], small_sem.at[0])
        wait_send(half_sum.at[late], small_sem.at[1])
        wait_send(recip.at[pl.ds(0, half - 1), late], small_sem.at[2])
    others = router_ref.at[pl.ds(0, ne - 1)]
    pltpu.make_async_remote_copy(
        others, others, router_send.at[1], router_col_sem, **shard(me)
    ).wait()
    for j in range(1, n):
        d = lax.rem(me + j, n)
        wait_recv(ready_ref.at[:, :, columns_of(d)], data_sem.at[d])


def update(train_down, other_down, weight, gain, n, ne):
    experts, inner, width = train_down.shape
    rows = inner // n
    r = unit_rows(rows)
    units = experts * (rows // r)
    lanes = -(-r // LANES) * LANES
    half = n // 2
    head = units if units <= GROUP else GROUP + units % GROUP
    groups = max(1, (units - head) // GROUP)
    result_bytes = 2 * experts * rows * width * n
    f32, bf16 = jnp.float32, jnp.bfloat16
    dma = pltpu.SemaphoreType.DMA
    return pl.pallas_call(
        functools.partial(update_kernel, n, ne, r, head),
        out_shape=(
            pltpu.VMEM((experts, rows, width * n), bf16),
            pltpu.VMEM((units, 1, lanes), f32),
            pltpu.VMEM((ne, weight.shape[0], width * n), bf16),
        ),
        in_specs=[
            pl.BlockSpec(memory_space=pl.ANY),
            pl.BlockSpec(memory_space=pl.ANY),
            pl.BlockSpec(memory_space=pltpu.VMEM),
            pl.BlockSpec(memory_space=pltpu.VMEM),
        ],
        out_specs=(pl.BlockSpec(memory_space=pltpu.VMEM),) * 3,
        scratch_shapes=[
            pltpu.VMEM((GROUP + 3, n, r, width), f32),
            pltpu.VMEM((GROUP + 3, n, r, width), bf16),
            pltpu.VMEM((RING, n - 1, r, width), bf16),
            pltpu.VMEM((half, units, 2, lanes), f32),
            pltpu.VMEM((head, n, half, 2, lanes), f32),
            pltpu.VMEM((half, units, 2, lanes), f32),
            pltpu.VMEM((units, 2, lanes), f32),
            pltpu.VMEM((units, 2, lanes), f32),
            pltpu.VMEM((half, units, 2, lanes), f32),
            dma((GROUP + 3,)),
            dma((GROUP + 3,)),
            dma((RING,)),
            dma((n,)),
            dma((4,)),
            dma((head,)),
            dma((groups,)),
            dma((groups,)),
            dma((groups,)),
            dma((2,)),
            dma,
            dma,
        ],
        compiler_params=pltpu.CompilerParams(
            collective_id=0,
            has_side_effects=True,
            vmem_limit_bytes=62 * 2**20 - result_bytes,
        ),
        name="update",
    )(
        train_down.reshape(experts, n, rows, width),
        other_down.reshape(experts, n, rows, width),
        weight,
        gain,
    )


def settle_kernel(
    ready_ref, scale_ref, router_ref, ready_out, scale_out, router_out, ready_sem
):
    experts, rows = scale_out.shape
    copies = [
        pltpu.make_async_copy(ready_ref.at[e], ready_out.at[e], ready_sem.at[e])
        for e in range(experts)
    ]
    for copy in copies:
        copy.start()
    steps = scale_ref.shape[0] // experts
    r = rows // steps
    for e in range(experts):
        runs = [scale_ref[e * steps + j][:, :r] for j in range(steps)]
        scale_out[e : e + 1, :] = jnp.concatenate(runs, axis=1)
    groups = [router_ref[g].astype(jnp.float32) for g in range(router_ref.shape[0])]
    router_out[...] = jnp.concatenate(groups, axis=0).astype(router_out.dtype)
    for copy in copies:
        copy.wait()


def settle(ready_down, scale, router):
    vmem = pl.BlockSpec(memory_space=pltpu.VMEM)
    experts, rows, width = ready_down.shape
    return pl.pallas_call(
        settle_kernel,
        out_shape=(
            jax.ShapeDtypeStruct(ready_down.shape, ready_down.dtype),
            jax.ShapeDtypeStruct((experts, rows), scale.dtype),
            jax.ShapeDtypeStruct((router.shape[0] * router.shape[1], width), router.dtype),
        ),
        in_specs=[vmem] * 3,
        out_specs=(pl.BlockSpec(memory_space=pl.ANY), vmem, vmem),
        scratch_shapes=[pltpu.SemaphoreType.DMA((experts,))],
        compiler_params=pltpu.CompilerParams(vmem_limit_bytes=8 * 2**20),
        name="settle",
    )(pltpu.with_memory_space_constraint(ready_down, pltpu.VMEM), scale, router)


def per_device(n, ne, train_down, other_down, router_weight, router_gain):
    ready_down, scale, router = update(
        train_down, other_down, router_weight.T, router_gain[None, :], n, ne
    )
    ready_down, scale_down, router = settle(ready_down, scale, router)
    return (ready_down, scale_down, router.T)


def solution(mesh):
    in_specs = (
        P("expert", None, "shard"),
        P("expert", None, "shard"),
        P("shard", "expert"),
        P("shard"),
    )
    out_specs = (P("expert", "shard", None), P("expert", "shard"), P())
    return jax.shard_map(
        functools.partial(per_device, mesh.shape["shard"], mesh.shape["expert"]),
        mesh=mesh,
        in_specs=in_specs,
        out_specs=out_specs,
        check_vma=False,
    )
```

```python
import functools

import jax
import jax.numpy as jnp
from jax import lax
from jax.experimental import pallas as pl
from jax.experimental.pallas import tpu as pltpu
from jax.sharding import PartitionSpec as P

LANES = 128
UNIT = 128
RING = 4
HEAD = 4
GROUP = 12
LAGS = (7, 4, 2)


def unit_rows(rows):
    fits = [r for r in range(16, UNIT + 1, 16) if rows % r == 0]
    return fits[-1] if fits else rows


def units_apart(units):
    head = min(HEAD, units)
    fits = [g for g in range(HEAD, GROUP + 1) if (units - head) % g == 0]
    return (head, fits[-1]) if fits else (units, 1)


def rows_to_lanes(column_sums):
    rows = column_sums.shape[0]
    out = []
    for start in range(0, rows, LANES):
        block = column_sums[start : min(start + LANES, rows)]
        if block.shape[0] < LANES:
            fill = jnp.zeros((LANES - block.shape[0], LANES), block.dtype)
            block = jnp.concatenate([block, fill], axis=0)
        out.append(jnp.sum(block.T, axis=0, keepdims=True))
    return jnp.concatenate(out, axis=1) if len(out) > 1 else out[0]


def lanes_to_rows(row, rows):
    out = []
    for start in range(0, rows, LANES):
        block = jnp.broadcast_to(row[:, start : start + LANES], (LANES, LANES)).T
        out.append(block[: min(LANES, rows - start)])
    return jnp.concatenate(out, axis=0) if len(out) > 1 else out[0]


def update_kernel(
    n, ne, r, head, group, late,
    train_ref, other_ref, weight_ref, gain_ref,
    ready_ref, scale_ref, router_ref, late_ref,
    train_buf, other_buf, stage, part, direct, first, half_sum, far_sum, recip,
    train_sem, other_sem, stage_sem, data_sem,
    small_sem, direct_sem, first_sem, far_sem, recip_sem,
    router_send, router_row_sem, router_col_sem,
):
    experts, _, rows, width = train_ref.shape
    steps = rows // r
    units = experts * steps
    groups = (units - head) // group
    half = n // 2
    ring_size = stage.shape[0]
    me, my_e = lax.axis_index("shard"), lax.axis_index("expert")
    place, side = lax.rem(me, half), lax.div(me, half)

    def shard(d):
        return {"device_id": {"shard": d}, "device_id_type": pl.DeviceIdType.MESH}

    def expert(d):
        return {"device_id": {"expert": d}, "device_id_type": pl.DeviceIdType.MESH}

    def wait_recv(ref, sem):
        pltpu.make_async_remote_copy(ref, ref, small_sem.at[0], sem, **shard(me)).wait_recv()

    def wait_send(ref, sem):
        pltpu.make_async_remote_copy(ref, ref, sem, data_sem.at[0], **shard(me)).wait_send()

    def where_is(k):
        start = lax.rem(k, steps) * r
        return lax.div(k, steps), pl.ds(pl.multiple_of(start, 8), r)

    def columns_of(d):
        return pl.ds(pl.multiple_of(d * width, LANES), width)

    def loads(k, slot):
        e, at = where_is(k)
        return (
            pltpu.make_async_copy(
                train_ref.at[e, :, at, :], train_buf.at[slot], train_sem.at[slot]
            ),
            pltpu.make_async_copy(
                other_ref.at[e, :, at, :], other_buf.at[slot], other_sem.at[slot]
            ),
        )

    def start_loads(k, slot):
        for copy in loads(k, slot):
            copy.start()

    def wait_loads(k, slot):
        for copy in loads(k, slot):
            copy.wait()

    def slot_of(k):
        return lax.rem(k, HEAD)

    def ahead_slot(k):
        return HEAD + lax.rem(k, HEAD)

    start_loads(0, 0)
    if units > 1:
        start_loads(1, 1)

    mine = columns_of(me)
    router_ref[my_e, :, mine] = (weight_ref[...] * gain_ref[...]).astype(router_ref.dtype)

    barrier = pltpu.get_barrier_semaphore()
    for j in range(1, n):
        pl.semaphore_signal(barrier, inc=1, **shard(lax.rem(me + j, n)))
    for j in range(1, ne):
        pl.semaphore_signal(barrier, inc=1, **expert(lax.rem(my_e + j, ne)))
    pl.semaphore_wait(barrier, n + ne - 2)

    def latest(slot, d):
        return train_buf[slot, d] + other_buf[slot, d].astype(jnp.float32)

    def sum_own(k, slot):
        wait_loads(k, slot)

        def body(q, carry):
            pair = []
            for t in (0, 1):
                x = latest(slot, t * half + q)
                x = x * x
                total = x[:, :LANES]
                for at in range(LANES, width, LANES):
                    total = total + x[:, at : at + LANES]
                pair.append(rows_to_lanes(total))
            part[q, k] = jnp.concatenate(pair, axis=0)
            return carry

        lax.fori_loop(0, half, body, 0)

    def own_side(pair):
        return jnp.where(side == 0, pair[..., 0:1, :], pair[..., 1:2, :])

    def send_direct(k):
        for q in range(half):
            direct[k, me, q] = part[q, k]
        for j in range(1, n):
            pltpu.make_async_remote_copy(
                src_ref=part.at[:, k],
                dst_ref=direct.at[k, me],
                send_sem=small_sem.at[3],
                recv_sem=direct_sem.at[k],
                **shard(lax.rem(me + (half + j - 1 if j <= half else j - half), n)),
            ).start()

    def sum_direct(k):
        wait_recv(direct.at[k, pl.ds(0, n - 1)], direct_sem.at[k])
        for q in range(half):
            total = direct[k, 0, q]
            for s in range(1, n):
                total = total + direct[k, s, q]
            scale = jnp.sqrt(total)
            recip[q, k] = 1.0 / scale

            @pl.when(place == q)
            def _(scale=scale):
                scale_ref[k] = own_side(scale)

    def units_of(g):
        return pl.ds(head + g * group, group)

    def sum_group(g):
        at = units_of(g)

        def body(j, carry):
            k = head + g * group + j
            sum_own(k, ahead_slot(k))

            @pl.when(k + HEAD < units)
            def _():
                start_loads(k + HEAD, ahead_slot(k))

            return carry

        lax.fori_loop(0, group, body, 0)
        first[place, at] = part[place, at]
        for j in range(1, half):
            q = lax.rem(place + j, half)
            pltpu.make_async_remote_copy(
                src_ref=part.at[q, at],
                dst_ref=first.at[place, at],
                send_sem=small_sem.at[0],
                recv_sem=first_sem.at[g],
                **shard(side * half + q),
            ).start()

    def sum_half(g):
        at = units_of(g)
        wait_recv(first.at[pl.ds(0, half - 1), at], first_sem.at[g])
        total = first[0, at]
        for q in range(1, half):
            total = total + first[q, at]
        half_sum[at] = total
        pltpu.make_async_remote_copy(
            src_ref=half_sum.at[at],
            dst_ref=far_sum.at[at],
            send_sem=small_sem.at[1],
            recv_sem=far_sem.at[g],
            **shard((1 - side) * half + place),
        ).start()

    def sum_all(g):
        at = units_of(g)
        wait_recv(far_sum.at[at], far_sem.at[g])
        scale = jnp.sqrt(half_sum[at] + far_sum[at])
        scale_ref[at] = own_side(scale)
        recip[place, at] = 1.0 / scale
        for j in range(1, half):
            q = lax.rem(place + j, half)
            pltpu.make_async_remote_copy(
                src_ref=recip.at[place, at],
                dst_ref=recip.at[place, at],
                send_sem=small_sem.at[2],
                recv_sem=recip_sem.at[g],
                **shard(side * half + q),
            ).start()

    def wait_stage(slot):
        wait_send(stage.at[slot, pl.ds(0, n - 1)], stage_sem.at[slot])

    def send(k):
        slot, ring = slot_of(k), lax.rem(k, ring_size)
        e, at = where_is(k)

        @pl.when(k >= head)
        def _():
            wait_loads(k, slot)

        @pl.when(k >= ring_size)
        def _():
            wait_stage(ring)

        is_late = k >= units - late

        def target(m):
            swapped = jnp.where(m < half, m + half - 1, m - half + 1)
            m = jnp.where(is_late & (m > 0), swapped, m)
            far = m < half
            t = jnp.where(far, 1 - side, side)
            q = lax.rem(place + jnp.where(far, m, m - half + 1), half)
            return t, q

        def piece(t, q):
            pair = recip[q, k]
            row = jnp.where(t == 0, pair[0:1], pair[1:2])
            factor = lanes_to_rows(row, r)
            factor = jnp.concatenate([factor] * (width // LANES), axis=1)
            return (latest(slot, t * half + q) * factor).astype(stage.dtype)

        def copy_to(m):
            t, q = target(m)
            return pltpu.make_async_remote_copy(
                src_ref=stage.at[ring, m],
                dst_ref=ready_ref.at[e, at, mine],
                send_sem=stage_sem.at[ring],
                recv_sem=data_sem.at[me],
                **shard(t * half + q),
            )

        @pl.when(is_late)
        def _():
            late_ref[k - (units - late)] = piece(*target(0))

        start = jnp.where(is_late, 1, 0)

        def body(m, carry):
            stage[ring, m] = piece(*target(m))

            @pl.when(m > start)
            def _():
                copy_to(m - 1).start()

            return carry

        lax.fori_loop(start, n - 1, body, 0)
        ready_ref[e, at, mine] = piece(side, place)
        copy_to(n - 2).start()

    for k in range(2, min(HEAD, units)):
        start_loads(k, k)
    for k in range(head):
        sum_own(k, slot_of(k))
        send_direct(k)
        if k + HEAD < head:
            start_loads(k + HEAD, k)
    for k in range(head, min(head + HEAD, units)):
        start_loads(k, ahead_slot(k))

    def step(i, carry):
        def at_lag(lag, start):
            g = jnp.where(i == start, 0, lax.div(i + lag - head, group))
            due = (i == start) | (
                (i + lag >= head + group) & (lax.rem(i + lag - head, group) == 0)
            )
            return g, due & (g < groups)

        if groups > 0:
            g, due = at_lag(LAGS[2], 3)

            @pl.when(due)
            def _():
                sum_all(g)

            g, due = at_lag(LAGS[1], 2)

            @pl.when(due)
            def _():
                sum_half(g)

        @pl.when(i < head)
        def _():
            sum_direct(i)

        if groups > 0:

            @pl.when((i >= head) & (lax.rem(i - head, group) == 0))
            def _():
                g = lax.div(i - head, group)
                wait_recv(recip.at[pl.ds(0, half - 1), units_of(g)], recip_sem.at[g])

        send(i)

        @pl.when((i + HEAD >= head) & (i + HEAD < units))
        def _():
            start_loads(i + HEAD, slot_of(i))

        if groups > 0:
            g, due = at_lag(LAGS[0], 0)

            @pl.when(due)
            def _():
                sum_group(g)

        return carry

    def send_router():
        for j in range(1, n):
            pltpu.make_async_remote_copy(
                src_ref=router_ref.at[my_e, :, mine],
                dst_ref=router_ref.at[my_e, :, mine],
                send_sem=router_send.at[0],
                recv_sem=router_row_sem,
                **shard(lax.rem(me + j, n)),
            ).start()

    lax.fori_loop(0, 1, step, 0)
    send_router()
    lax.fori_loop(1, units, step, 0)

    others = router_ref.at[0, :, pl.ds(0, (n - 1) * width)]
    pltpu.make_async_remote_copy(
        others, others, router_send.at[0], router_row_sem, **shard(me)
    ).wait()
    for j in range(1, ne):
        pltpu.make_async_remote_copy(
            src_ref=router_ref.at[my_e],
            dst_ref=router_ref.at[my_e],
            send_sem=router_send.at[1],
            recv_sem=router_col_sem,
            **expert(lax.rem(my_e + j, ne)),
        ).start()

    for k in range(max(0, units - ring_size), units):
        if k < units - late:
            wait_stage(k % ring_size)
        else:
            wait_send(stage.at[k % ring_size, pl.ds(1, n - 2)], stage_sem.at[k % ring_size])
    wait_send(direct.at[:, pl.ds(0, n - 1)], small_sem.at[3])
    if groups > 0:
        grouped = pl.ds(head, groups * group)
        wait_send(part.at[pl.ds(0, half - 1), grouped], small_sem.at[0])
        wait_send(half_sum.at[grouped], small_sem.at[1])
        wait_send(recip.at[pl.ds(0, half - 1), grouped], small_sem.at[2])
    others = router_ref.at[pl.ds(0, ne - 1)]
    pltpu.make_async_remote_copy(
        others, others, router_send.at[1], router_col_sem, **shard(me)
    ).wait()
    for j in range(1, n):
        d = lax.rem(me + j, n)
        if j != half:
            wait_recv(ready_ref.at[:, :, columns_of(d)], data_sem.at[d])
            continue
        early = rows - late // experts * r
        if early > 0:
            wait_recv(ready_ref.at[:, pl.ds(0, early), columns_of(d)], data_sem.at[d])


def update(train_down, other_down, weight, gain, n, ne):
    experts, inner, width = train_down.shape
    rows = inner // n
    r = unit_rows(rows)
    units = experts * (rows // r)
    lanes = -(-r // LANES) * LANES
    half = n // 2
    head, group = units_apart(units)
    groups = max(1, (units - head) // group)
    late = experts
    ring_size = max(RING, late)
    result_bytes = 2 * experts * rows * width * n
    f32, bf16 = jnp.float32, jnp.bfloat16
    dma = pltpu.SemaphoreType.DMA
    return pl.pallas_call(
        functools.partial(update_kernel, n, ne, r, head, group, late),
        out_shape=(
            pltpu.VMEM((experts, rows, width * n), bf16),
            pltpu.VMEM((units, 1, lanes), f32),
            pltpu.VMEM((ne, weight.shape[0], width * n), bf16),
            pltpu.VMEM((late, r, width), bf16),
        ),
        in_specs=[
            pl.BlockSpec(memory_space=pl.ANY),
            pl.BlockSpec(memory_space=pl.ANY),
            pl.BlockSpec(memory_space=pltpu.VMEM),
            pl.BlockSpec(memory_space=pltpu.VMEM),
        ],
        out_specs=(pl.BlockSpec(memory_space=pltpu.VMEM),) * 4,
        scratch_shapes=[
            pltpu.VMEM((2 * HEAD, n, r, width), f32),
            pltpu.VMEM((2 * HEAD, n, r, width), bf16),
            pltpu.VMEM((ring_size, n - 1, r, width), bf16),
            pltpu.VMEM((half, units, 2, lanes), f32),
            pltpu.VMEM((head, n, half, 2, lanes), f32),
            pltpu.VMEM((half, units, 2, lanes), f32),
            pltpu.VMEM((units, 2, lanes), f32),
            pltpu.VMEM((units, 2, lanes), f32),
            pltpu.VMEM((half, units, 2, lanes), f32),
            dma((2 * HEAD,)),
            dma((2 * HEAD,)),
            dma((ring_size,)),
            dma((n,)),
            dma((4,)),
            dma((head,)),
            dma((groups,)),
            dma((groups,)),
            dma((groups,)),
            dma((2,)),
            dma,
            dma,
        ],
        compiler_params=pltpu.CompilerParams(
            collective_id=0,
            has_side_effects=True,
            vmem_limit_bytes=62 * 2**20 - result_bytes,
        ),
        name="update",
    )(
        train_down.reshape(experts, n, rows, width),
        other_down.reshape(experts, n, rows, width),
        weight,
        gain,
    )


def settle_kernel(
    ready_ref, scale_ref, router_ref, ready_out, scale_out, router_out,
    scale_buf, router_buf, ready_sem, small_sem,
):
    experts, rows = scale_buf.shape
    steps = scale_ref.shape[0] // experts
    r = rows // steps
    copies = [
        pltpu.make_async_copy(
            ready_ref.at[e, pl.ds(j * r, r)], ready_out.at[e, pl.ds(j * r, r)], ready_sem.at[e]
        )
        for e in range(experts)
        for j in range(steps)
    ]
    for copy in copies:
        copy.start()
    for e in range(experts):
        runs = [scale_ref[e * steps + j][:, :r] for j in range(steps)]
        scale_buf[e : e + 1, :] = jnp.concatenate(runs, axis=1)
    groups = [router_ref[g].astype(jnp.float32) for g in range(router_ref.shape[0])]
    router_buf[...] = jnp.concatenate(groups, axis=0).astype(router_buf.dtype)
    small = [
        pltpu.make_async_copy(scale_buf, scale_out, small_sem.at[0]),
        pltpu.make_async_copy(router_buf, router_out, small_sem.at[1]),
    ]
    for copy in small:
        copy.start()
    for copy in small + copies:
        copy.wait()


def settle(ready_down, scale, router):
    vmem, hbm = pl.BlockSpec(memory_space=pltpu.VMEM), pl.BlockSpec(memory_space=pl.ANY)
    experts, rows, width = ready_down.shape
    small = [
        ((experts, rows), scale.dtype),
        ((router.shape[0] * router.shape[1], width), router.dtype),
    ]
    return pl.pallas_call(
        settle_kernel,
        out_shape=(jax.ShapeDtypeStruct(ready_down.shape, ready_down.dtype),)
        + tuple(jax.ShapeDtypeStruct(*x) for x in small),
        in_specs=[vmem] * 3,
        out_specs=(hbm,) * 3,
        scratch_shapes=[pltpu.VMEM(*x) for x in small]
        + [pltpu.SemaphoreType.DMA((experts,)), pltpu.SemaphoreType.DMA((2,))],
        compiler_params=pltpu.CompilerParams(vmem_limit_bytes=8 * 2**20),
        cost_estimate=pl.CostEstimate(
            flops=10**8, bytes_accessed=2 * ready_down.size, transcendentals=0
        ),
        name="settle",
    )(pltpu.with_memory_space_constraint(ready_down, pltpu.VMEM), scale, router)


def place_late_kernel(n, late_ref, _, ready_ref, sem):
    late, r, width = late_ref.shape
    experts, rows, _ = ready_ref.shape
    steps = rows // r
    far = lax.rem(lax.axis_index("shard") + n // 2, n)
    columns = pl.ds(pl.multiple_of(far * width, LANES), width)
    copies = []
    for j in range(late):
        e, at = divmod(experts * steps - late + j, steps)
        there = ready_ref.at[e, pl.ds(at * r, r), columns]
        copies.append(pltpu.make_async_copy(late_ref.at[j], there, sem.at[j]))
    for copy in copies:
        copy.start()
    for copy in copies:
        copy.wait()


def place_late(late_down, ready_down, n):
    hbm = pl.BlockSpec(memory_space=pl.ANY)
    return pl.pallas_call(
        functools.partial(place_late_kernel, n),
        out_shape=jax.ShapeDtypeStruct(ready_down.shape, ready_down.dtype),
        in_specs=[pl.BlockSpec(memory_space=pltpu.VMEM), hbm],
        out_specs=hbm,
        scratch_shapes=[pltpu.SemaphoreType.DMA((late_down.shape[0],))],
        input_output_aliases={1: 0},
        compiler_params=pltpu.CompilerParams(vmem_limit_bytes=8 * 2**20),
        name="place_late",
    )(late_down, ready_down)


def per_device(n, ne, train_down, other_down, router_weight, router_gain):
    ready_down, scale, router, late_down = update(
        train_down, other_down, router_weight.T, router_gain[None, :], n, ne
    )
    late_down = lax.ppermute(late_down, "shard", [(s, (s + n // 2) % n) for s in range(n)])
    ready_down, scale_down, router = settle(ready_down, scale, router)
    ready_down = place_late(late_down, ready_down, n)
    return (ready_down, scale_down, router.T)


def solution(mesh):
    in_specs = (
        P("expert", None, "shard"),
        P("expert", None, "shard"),
        P("shard", "expert"),
        P("shard"),
    )
    out_specs = (P("expert", "shard", None), P("expert", "shard"), P())
    return jax.shard_map(
        functools.partial(per_device, mesh.shape["shard"], mesh.shape["expert"]),
        mesh=mesh,
        in_specs=in_specs,
        out_specs=out_specs,
        check_vma=False,
    )
```

```python
import functools

import jax
import jax.numpy as jnp
from jax import lax
from jax.experimental import pallas as pl
from jax.experimental.pallas import tpu as pltpu
from jax.sharding import PartitionSpec as P

LANES = 128
UNIT = 128
RING = 6
HEAD = 4
GROUP = 12
LAGS = (7, 4, 2)


def unit_rows(rows):
    fits = [r for r in range(16, UNIT + 1, 16) if rows % r == 0]
    return fits[-1] if fits else rows


def units_apart(units):
    head = min(HEAD, units)
    fits = [g for g in range(HEAD, GROUP + 1) if (units - head) % g == 0]
    return (head, fits[-1]) if fits else (units, 1)


def rows_to_lanes(column_sums):
    rows = column_sums.shape[0]
    out = []
    for start in range(0, rows, LANES):
        block = column_sums[start : min(start + LANES, rows)]
        if block.shape[0] < LANES:
            fill = jnp.zeros((LANES - block.shape[0], LANES), block.dtype)
            block = jnp.concatenate([block, fill], axis=0)
        out.append(jnp.sum(block.T, axis=0, keepdims=True))
    return jnp.concatenate(out, axis=1) if len(out) > 1 else out[0]


def lanes_to_rows(row, rows):
    out = []
    for start in range(0, rows, LANES):
        block = jnp.broadcast_to(row[:, start : start + LANES], (LANES, LANES)).T
        out.append(block[: min(LANES, rows - start)])
    return jnp.concatenate(out, axis=0) if len(out) > 1 else out[0]


def update_kernel(
    n, ne, r, head, group, late,
    train_ref, other_ref, weight_ref, gain_ref,
    ready_ref, scale_ref, router_ref, late_ref,
    train_buf, other_buf, stage, part, direct, first, half_sum, far_sum, recip,
    train_sem, other_sem, stage_sem, data_sem,
    small_sem, direct_sem, first_sem, far_sem, recip_sem,
    router_send, router_row_sem, router_col_sem,
):
    experts, _, rows, width = train_ref.shape
    steps = rows // r
    units = experts * steps
    groups = (units - head) // group
    half = n // 2
    ring_size = stage.shape[0]
    me, my_e = lax.axis_index("shard"), lax.axis_index("expert")
    place, side = lax.rem(me, half), lax.div(me, half)

    def shard(d):
        return {"device_id": {"shard": d}, "device_id_type": pl.DeviceIdType.MESH}

    def expert(d):
        return {"device_id": {"expert": d}, "device_id_type": pl.DeviceIdType.MESH}

    def wait_recv(ref, sem):
        pltpu.make_async_remote_copy(ref, ref, small_sem.at[0], sem, **shard(me)).wait_recv()

    def wait_send(ref, sem):
        pltpu.make_async_remote_copy(ref, ref, sem, data_sem.at[0], **shard(me)).wait_send()

    def where_is(k):
        start = lax.rem(k, steps) * r
        return lax.div(k, steps), pl.ds(pl.multiple_of(start, 8), r)

    def columns_of(d):
        return pl.ds(pl.multiple_of(d * width, LANES), width)

    def loads(k, slot):
        e, at = where_is(k)
        return (
            pltpu.make_async_copy(
                train_ref.at[e, :, at, :], train_buf.at[slot], train_sem.at[slot]
            ),
            pltpu.make_async_copy(
                other_ref.at[e, :, at, :], other_buf.at[slot], other_sem.at[slot]
            ),
        )

    def start_loads(k, slot):
        for copy in loads(k, slot):
            copy.start()

    def wait_loads(k, slot):
        for copy in loads(k, slot):
            copy.wait()

    def slot_of(k):
        return lax.rem(k, HEAD)

    def ahead_slot(k):
        return HEAD + lax.rem(k, HEAD)

    start_loads(0, 0)
    if units > 1:
        start_loads(1, 1)

    mine = columns_of(me)
    router_ref[my_e, :, mine] = (weight_ref[...] * gain_ref[...]).astype(router_ref.dtype)

    barrier = pltpu.get_barrier_semaphore()
    for j in range(1, n):
        pl.semaphore_signal(barrier, inc=1, **shard(lax.rem(me + j, n)))
    for j in range(1, ne):
        pl.semaphore_signal(barrier, inc=1, **expert(lax.rem(my_e + j, ne)))
    pl.semaphore_wait(barrier, n + ne - 2)

    def latest(slot, d):
        return train_buf[slot, d] + other_buf[slot, d].astype(jnp.float32)

    def sum_own(k, slot):
        wait_loads(k, slot)

        def body(q, carry):
            pair = []
            for t in (0, 1):
                x = latest(slot, t * half + q)
                x = x * x
                total = x[:, :LANES]
                for at in range(LANES, width, LANES):
                    total = total + x[:, at : at + LANES]
                pair.append(rows_to_lanes(total))
            part[q, k] = jnp.concatenate(pair, axis=0)
            return carry

        lax.fori_loop(0, half, body, 0)

    def own_side(pair):
        return jnp.where(side == 0, pair[..., 0:1, :], pair[..., 1:2, :])

    def send_direct(k):
        for q in range(half):
            direct[k, me, q] = part[q, k]
        for j in range(1, n):
            pltpu.make_async_remote_copy(
                src_ref=part.at[:, k],
                dst_ref=direct.at[k, me],
                send_sem=small_sem.at[3],
                recv_sem=direct_sem.at[k],
                **shard(lax.rem(me + (half + j - 1 if j <= half else j - half), n)),
            ).start()

    def sum_direct(k):
        wait_recv(direct.at[k, pl.ds(0, n - 1)], direct_sem.at[k])
        for q in range(half):
            total = direct[k, 0, q]
            for s in range(1, n):
                total = total + direct[k, s, q]
            scale = jnp.sqrt(total)
            recip[q, k] = 1.0 / scale

            @pl.when(place == q)
            def _(scale=scale):
                scale_ref[k] = own_side(scale)

    def units_of(g):
        return pl.ds(head + g * group, group)

    def sum_group(g):
        at = units_of(g)

        def body(j, carry):
            k = head + g * group + j
            sum_own(k, ahead_slot(k))

            @pl.when(k + HEAD < units)
            def _():
                start_loads(k + HEAD, ahead_slot(k))

            return carry

        lax.fori_loop(0, group, body, 0)
        first[place, at] = part[place, at]
        for j in range(1, half):
            q = lax.rem(place + j, half)
            pltpu.make_async_remote_copy(
                src_ref=part.at[q, at],
                dst_ref=first.at[place, at],
                send_sem=small_sem.at[0],
                recv_sem=first_sem.at[g],
                **shard(side * half + q),
            ).start()

    def sum_half(g):
        at = units_of(g)
        wait_recv(first.at[pl.ds(0, half - 1), at], first_sem.at[g])
        total = first[0, at]
        for q in range(1, half):
            total = total + first[q, at]
        half_sum[at] = total
        pltpu.make_async_remote_copy(
            src_ref=half_sum.at[at],
            dst_ref=far_sum.at[at],
            send_sem=small_sem.at[1],
            recv_sem=far_sem.at[g],
            **shard((1 - side) * half + place),
        ).start()

    def sum_all(g):
        at = units_of(g)
        wait_recv(far_sum.at[at], far_sem.at[g])
        scale = jnp.sqrt(half_sum[at] + far_sum[at])
        scale_ref[at] = own_side(scale)
        recip[place, at] = 1.0 / scale
        for j in range(1, half):
            q = lax.rem(place + j, half)
            pltpu.make_async_remote_copy(
                src_ref=recip.at[place, at],
                dst_ref=recip.at[place, at],
                send_sem=small_sem.at[2],
                recv_sem=recip_sem.at[g],
                **shard(side * half + q),
            ).start()

    def wait_stage(slot):
        wait_send(stage.at[slot, pl.ds(0, n - 1)], stage_sem.at[slot])

    def send(k):
        slot, ring = slot_of(k), lax.rem(k, ring_size)
        e, at = where_is(k)

        @pl.when(k >= head)
        def _():
            wait_loads(k, slot)

        @pl.when(k >= ring_size)
        def _():
            wait_stage(ring)

        is_late = k >= units - late

        def target(m):
            swapped = jnp.where(m < half, m + half - 1, m - half + 1)
            m = jnp.where(is_late & (m > 0), swapped, m)
            far = m < half
            t = jnp.where(far, 1 - side, side)
            turn = jnp.where(far & jnp.logical_not(is_late), lax.rem(my_e, 2) * (half // 2), 0)
            q = lax.rem(place + turn + jnp.where(far, m, m - half + 1), half)
            return t, q

        def piece(t, q):
            pair = recip[q, k]
            row = jnp.where(t == 0, pair[0:1], pair[1:2])
            factor = lanes_to_rows(row, r)
            factor = jnp.concatenate([factor] * (width // LANES), axis=1)
            return (latest(slot, t * half + q) * factor).astype(stage.dtype)

        def copy_to(m):
            t, q = target(m)
            return pltpu.make_async_remote_copy(
                src_ref=stage.at[ring, m],
                dst_ref=ready_ref.at[e, at, mine],
                send_sem=stage_sem.at[ring],
                recv_sem=data_sem.at[me],
                **shard(t * half + q),
            )

        @pl.when(is_late)
        def _():
            late_ref[k - (units - late)] = piece(*target(0))

        start = jnp.where(is_late, 1, 0)

        def body(m, carry):
            stage[ring, m] = piece(*target(m))

            @pl.when(m > start)
            def _():
                copy_to(m - 1).start()

            return carry

        lax.fori_loop(start, n - 1, body, 0)
        ready_ref[e, at, mine] = piece(side, place)
        copy_to(n - 2).start()

    for k in range(2, min(HEAD, units)):
        start_loads(k, k)
    for k in range(head):
        sum_own(k, slot_of(k))
        send_direct(k)
        if k + HEAD < head:
            start_loads(k + HEAD, k)
    for k in range(head, min(head + HEAD, units)):
        start_loads(k, ahead_slot(k))

    def step(i, carry):
        def at_lag(lag, start):
            g = jnp.where(i == start, 0, lax.div(i + lag - head, group))
            due = (i == start) | (
                (i + lag >= head + group) & (lax.rem(i + lag - head, group) == 0)
            )
            return g, due & (g < groups)

        if groups > 0:
            g, due = at_lag(LAGS[2], 3)

            @pl.when(due)
            def _():
                sum_all(g)

            g, due = at_lag(LAGS[1], 2)

            @pl.when(due)
            def _():
                sum_half(g)

        @pl.when(i < head)
        def _():
            sum_direct(i)

        if groups > 0:

            @pl.when((i >= head) & (lax.rem(i - head, group) == 0))
            def _():
                g = lax.div(i - head, group)
                wait_recv(recip.at[pl.ds(0, half - 1), units_of(g)], recip_sem.at[g])

        send(i)

        @pl.when((i + HEAD >= head) & (i + HEAD < units))
        def _():
            start_loads(i + HEAD, slot_of(i))

        if groups > 0:
            g, due = at_lag(LAGS[0], 0)

            @pl.when(due)
            def _():
                sum_group(g)

        return carry

    def send_router():
        for j in range(1, n):
            pltpu.make_async_remote_copy(
                src_ref=router_ref.at[my_e, :, mine],
                dst_ref=router_ref.at[my_e, :, mine],
                send_sem=router_send.at[0],
                recv_sem=router_row_sem,
                **shard(lax.rem(me + j, n)),
            ).start()

    lax.fori_loop(0, 1, step, 0)
    send_router()
    lax.fori_loop(1, units, step, 0)

    others = router_ref.at[0, :, pl.ds(0, (n - 1) * width)]
    pltpu.make_async_remote_copy(
        others, others, router_send.at[0], router_row_sem, **shard(me)
    ).wait()
    for j in range(1, ne):
        pltpu.make_async_remote_copy(
            src_ref=router_ref.at[my_e],
            dst_ref=router_ref.at[my_e],
            send_sem=router_send.at[1],
            recv_sem=router_col_sem,
            **expert(lax.rem(my_e + j, ne)),
        ).start()

    for k in range(max(0, units - ring_size), units):
        if k < units - late:
            wait_stage(k % ring_size)
        else:
            wait_send(stage.at[k % ring_size, pl.ds(1, n - 2)], stage_sem.at[k % ring_size])
    wait_send(direct.at[:, pl.ds(0, n - 1)], small_sem.at[3])
    if groups > 0:
        grouped = pl.ds(head, groups * group)
        wait_send(part.at[pl.ds(0, half - 1), grouped], small_sem.at[0])
        wait_send(half_sum.at[grouped], small_sem.at[1])
        wait_send(recip.at[pl.ds(0, half - 1), grouped], small_sem.at[2])
    others = router_ref.at[pl.ds(0, ne - 1)]
    pltpu.make_async_remote_copy(
        others, others, router_send.at[1], router_col_sem, **shard(me)
    ).wait()
    for j in range(1, n):
        d = lax.rem(me + j, n)
        if j != half:
            wait_recv(ready_ref.at[:, :, columns_of(d)], data_sem.at[d])
            continue
        early = rows - late // experts * r
        if early > 0:
            wait_recv(ready_ref.at[:, pl.ds(0, early), columns_of(d)], data_sem.at[d])


def update(train_down, other_down, weight, gain, n, ne):
    experts, inner, width = train_down.shape
    rows = inner // n
    r = unit_rows(rows)
    units = experts * (rows // r)
    lanes = -(-r // LANES) * LANES
    half = n // 2
    head, group = units_apart(units)
    groups = max(1, (units - head) // group)
    late = experts
    ring_size = max(RING, late)
    result_bytes = 2 * experts * rows * width * n
    f32, bf16 = jnp.float32, jnp.bfloat16
    dma = pltpu.SemaphoreType.DMA
    return pl.pallas_call(
        functools.partial(update_kernel, n, ne, r, head, group, late),
        out_shape=(
            pltpu.VMEM((experts, rows, width * n), bf16),
            pltpu.VMEM((units, 1, lanes), f32),
            pltpu.VMEM((ne, weight.shape[0], width * n), bf16),
            pltpu.VMEM((late, r, width), bf16),
        ),
        in_specs=[
            pl.BlockSpec(memory_space=pl.ANY),
            pl.BlockSpec(memory_space=pl.ANY),
            pl.BlockSpec(memory_space=pltpu.VMEM),
            pl.BlockSpec(memory_space=pltpu.VMEM),
        ],
        out_specs=(pl.BlockSpec(memory_space=pltpu.VMEM),) * 4,
        scratch_shapes=[
            pltpu.VMEM((2 * HEAD, n, r, width), f32),
            pltpu.VMEM((2 * HEAD, n, r, width), bf16),
            pltpu.VMEM((ring_size, n - 1, r, width), bf16),
            pltpu.VMEM((half, units, 2, lanes), f32),
            pltpu.VMEM((head, n, half, 2, lanes), f32),
            pltpu.VMEM((half, units, 2, lanes), f32),
            pltpu.VMEM((units, 2, lanes), f32),
            pltpu.VMEM((units, 2, lanes), f32),
            pltpu.VMEM((half, units, 2, lanes), f32),
            dma((2 * HEAD,)),
            dma((2 * HEAD,)),
            dma((ring_size,)),
            dma((n,)),
            dma((4,)),
            dma((head,)),
            dma((groups,)),
            dma((groups,)),
            dma((groups,)),
            dma((2,)),
            dma,
            dma,
        ],
        compiler_params=pltpu.CompilerParams(
            collective_id=0,
            has_side_effects=True,
            vmem_limit_bytes=62 * 2**20 - result_bytes,
        ),
        name="update",
    )(
        train_down.reshape(experts, n, rows, width),
        other_down.reshape(experts, n, rows, width),
        weight,
        gain,
    )


def settle_kernel(
    ready_ref, scale_ref, router_ref, ready_out, scale_out, router_out,
    scale_buf, router_buf, ready_sem, small_sem,
):
    experts, rows = scale_buf.shape
    steps = scale_ref.shape[0] // experts
    r = rows // steps
    copies = [
        pltpu.make_async_copy(
            ready_ref.at[e, pl.ds(j * r, r)], ready_out.at[e, pl.ds(j * r, r)], ready_sem.at[e]
        )
        for e in range(experts)
        for j in range(steps)
    ]
    for copy in copies:
        copy.start()
    for e in range(experts):
        runs = [scale_ref[e * steps + j][:, :r] for j in range(steps)]
        scale_buf[e : e + 1, :] = jnp.concatenate(runs, axis=1)
    groups = [router_ref[g].astype(jnp.float32) for g in range(router_ref.shape[0])]
    router_buf[...] = jnp.concatenate(groups, axis=0).astype(router_buf.dtype)
    small = [
        pltpu.make_async_copy(scale_buf, scale_out, small_sem.at[0]),
        pltpu.make_async_copy(router_buf, router_out, small_sem.at[1]),
    ]
    for copy in small:
        copy.start()
    for copy in small + copies:
        copy.wait()


def settle(ready_down, scale, router):
    vmem, hbm = pl.BlockSpec(memory_space=pltpu.VMEM), pl.BlockSpec(memory_space=pl.ANY)
    experts, rows, width = ready_down.shape
    small = [
        ((experts, rows), scale.dtype),
        ((router.shape[0] * router.shape[1], width), router.dtype),
    ]
    return pl.pallas_call(
        settle_kernel,
        out_shape=(jax.ShapeDtypeStruct(ready_down.shape, ready_down.dtype),)
        + tuple(jax.ShapeDtypeStruct(*x) for x in small),
        in_specs=[vmem] * 3,
        out_specs=(hbm,) * 3,
        scratch_shapes=[pltpu.VMEM(*x) for x in small]
        + [pltpu.SemaphoreType.DMA((experts,)), pltpu.SemaphoreType.DMA((2,))],
        compiler_params=pltpu.CompilerParams(vmem_limit_bytes=8 * 2**20),
        cost_estimate=pl.CostEstimate(
            flops=10**8, bytes_accessed=2 * ready_down.size, transcendentals=0
        ),
        name="settle",
    )(pltpu.with_memory_space_constraint(ready_down, pltpu.VMEM), scale, router)


def place_late_kernel(n, late_ref, _, ready_ref, sem):
    late, r, width = late_ref.shape
    experts, rows, _ = ready_ref.shape
    steps = rows // r
    far = lax.rem(lax.axis_index("shard") + n // 2, n)
    columns = pl.ds(pl.multiple_of(far * width, LANES), width)
    copies = []
    for j in range(late):
        e, at = divmod(experts * steps - late + j, steps)
        there = ready_ref.at[e, pl.ds(at * r, r), columns]
        copies.append(pltpu.make_async_copy(late_ref.at[j], there, sem.at[j]))
    for copy in copies:
        copy.start()
    for copy in copies:
        copy.wait()


def place_late(late_down, ready_down, n):
    hbm = pl.BlockSpec(memory_space=pl.ANY)
    return pl.pallas_call(
        functools.partial(place_late_kernel, n),
        out_shape=jax.ShapeDtypeStruct(ready_down.shape, ready_down.dtype),
        in_specs=[pl.BlockSpec(memory_space=pltpu.VMEM), hbm],
        out_specs=hbm,
        scratch_shapes=[pltpu.SemaphoreType.DMA((late_down.shape[0],))],
        input_output_aliases={1: 0},
        compiler_params=pltpu.CompilerParams(vmem_limit_bytes=8 * 2**20),
        name="place_late",
    )(late_down, ready_down)


def per_device(n, ne, train_down, other_down, router_weight, router_gain):
    ready_down, scale, router, late_down = update(
        train_down, other_down, router_weight.T, router_gain[None, :], n, ne
    )
    late_down = lax.ppermute(late_down, "shard", [(s, (s + n // 2) % n) for s in range(n)])
    ready_down, scale_down, router = settle(ready_down, scale, router)
    ready_down = place_late(late_down, ready_down, n)
    return (ready_down, scale_down, router.T)


def solution(mesh):
    in_specs = (
        P("expert", None, "shard"),
        P("expert", None, "shard"),
        P("shard", "expert"),
        P("shard"),
    )
    out_specs = (P("expert", "shard", None), P("expert", "shard"), P())
    return jax.shard_map(
        functools.partial(per_device, mesh.shape["shard"], mesh.shape["expert"]),
        mesh=mesh,
        in_specs=in_specs,
        out_specs=out_specs,
        check_vma=False,
    )
```
